32 devices in a mesh: shard: 8 (over z, x), model: 4 (over y, core).
Axes of the slice: x: 2, y: 2, z: 4, core: 2. Of those that a mesh axis runs over, the one named last changes fastest.
Arguments:
- grad_stack: float32 [64, 128, 2048], P(None, 'shard', 'model'), may hold values from -6 to 6
- moment_stack: float32 [64, 128, 2048], P(None, 'shard', 'model'), may hold values from -6 to 6
- weight_stack: float32 [64, 128, 2048], P(None, 'shard', 'model'), may hold values from -0.1875 to 0.1875
Outputs:
- new_weights: float32 [64, 128, 2048], P(None, 'shard', 'model')
- new_momentum: float32 [64, 128, 2048], P(None, 'shard', 'model')
The draws below stay inside these ranges and needn't reach their ends.
All inputs are finite; a program needn't handle non-finite values.
Results may differ from the reference program's by a relative error of at most 0.00021.
Values sent between devices are 32-bit elements; how exact they have to be, the bound alone decides.
A program may use at most 64 MiB of HBM per device.

```python
import jax
import jax.numpy as jnp
from jax import lax

SIDE = 128
WIDE = 2048
MATS = 64
ITERS = 5


def shard_levels(own_key, extent, pieces, least, high):
    def one(position, parts):
        steps = jax.random.uniform(jax.random.fold_in(jax.random.fold_in(own_key, 6), position), (parts,), jnp.float32, least / len(pieces), high / len(pieces))
        return jnp.repeat(jnp.exp(steps), extent[position] // parts).reshape((-1,) + (1,) * (len(extent) - position - 1))

    loudness = one(*pieces[0])
    for cut in pieces[1:]:
        loudness = loudness * one(*cut)
    return loudness


def noise(rng, extent, width, most, shards=(), held_as=jnp.bfloat16):
    drawn = jax.random.normal(rng, extent, jnp.float32) * width
    if len(shards) > 0:
        drawn = shard_levels(rng, extent, shards, -0.22, 0.18) * drawn
    return jnp.clip(drawn, min=-most, max=most).astype(held_as)


def setup_inputs(seed: int = 0) -> dict:
    key_list = jax.random.split(jax.random.key(seed), 4)
    grad_stack = noise(key_list[0], (MATS, SIDE, WIDE), 1.0, 6.0, ((1, 8), (2, 4)), jnp.float32)
    moment_stack = noise(key_list[1], (MATS, SIDE, WIDE), 1.0, 6.0, ((1, 8), (2, 4)), jnp.float32)
    weight_stack = noise(key_list[2], (MATS, SIDE, WIDE), 0.03, 0.1875, ((1, 8), (2, 4)), jnp.float32)
    return {"grad_stack": grad_stack, "moment_stack": moment_stack, "weight_stack": weight_stack}


hold_rate = 0.95
learn_rate = 1.0
decay_rate = 0.1

def reference(grad_stack, moment_stack, weight_stack):
    new_momentum = hold_rate * moment_stack + grad_stack

    def orthogonal_one(stack):
        iterate = stack[None]
        iterate = iterate * lax.rsqrt(lax.optimization_barrier(jnp.sum(iterate * iterate, axis=(1, 2), keepdims=True)) + 1e-06)
        for step in range(ITERS):
            gram = jnp.einsum('mik,mjk->mij', iterate, iterate, precision=lax.Precision.HIGHEST)
            mixed = -4.775 * gram + 2.0315 * jnp.einsum('mij,mjk->mik', gram, gram, precision=lax.Precision.HIGHEST)
            iterate = 3.4445 * iterate + jnp.einsum('mij,mjk->mik', mixed, iterate, precision=lax.Precision.HIGHEST)
        return iterate[0]
    iterate = lax.map(orthogonal_one, new_momentum)
    new_weights = (1.0 - learn_rate * decay_rate) * weight_stack - learn_rate * iterate
    return (new_weights, new_momentum)
```

```python
import jax
import jax.numpy as jnp
from jax import lax
from jax.sharding import PartitionSpec as P

ITERS = 5


hold_rate = 0.95
learn_rate = 1.0
decay_rate = 0.1
HIGH = lax.Precision.HIGHEST


def batched(a, b):
    return jnp.einsum("mij,mjk->mik", a, b, precision=HIGH)


def polynomial(gram):
    size = jnp.trace(gram, axis1=1, axis2=2)[:, None, None]
    scale = lax.rsqrt(size + 1e-06)
    gram = gram * (scale * scale)
    eye = jnp.eye(gram.shape[-1], dtype=gram.dtype)
    total = None
    for step in range(ITERS):
        factor = 3.4445 * eye + (-4.775 * gram + 2.0315 * batched(gram, gram))
        total = factor if total is None else batched(factor, total)
        if step < ITERS - 1:
            gram = batched(factor, batched(gram, factor))
    return total * scale


def on_device(grad_stack, moment_stack, weight_stack):
    new_momentum = hold_rate * moment_stack + grad_stack
    moved = lax.all_to_all(new_momentum, "shard", split_axis=0, concat_axis=1, tiled=True)
    part = jnp.einsum("mik,mjk->mij", moved, moved, precision=HIGH)
    parts = lax.axis_size("model")
    part = part.reshape((parts, part.shape[0] // parts) + part.shape[1:])
    gram = jnp.sum(lax.all_to_all(part, "model", split_axis=0, concat_axis=0), axis=0)
    mixed = lax.all_gather(polynomial(gram), "model", axis=0, tiled=True)
    iterate = batched(mixed, moved)
    back = lax.all_to_all(iterate, "shard", split_axis=1, concat_axis=0, tiled=True)
    new_weights = (1.0 - learn_rate * decay_rate) * weight_stack - learn_rate * back
    return (new_weights, new_momentum)


def solution(mesh):
    in_specs = (P(None, "shard", "model"), P(None, "shard", "model"), P(None, "shard", "model"))
    out_specs = (P(None, "shard", "model"), P(None, "shard", "model"))
    return jax.shard_map(
        on_device, mesh=mesh, in_specs=in_specs, out_specs=out_specs, check_vma=False
    )
```
